256 devices in a mesh: space: 32 (over x, z_hi, core), mem: 8 (over y, z_lo).
Axes of the slice: x: 4, y: 4, z: 8 (z_hi: 4, z_lo: 2; z = z_hi * 2 + z_lo), core: 2. Of those that a mesh axis runs over, the one named last changes fastest.
Arguments:
- ensemble: bfloat16 [32, 32, 512, 1536], P('mem', None, 'space'), may hold values from -12 to 12
- vector: bfloat16 [32, 512, 1536], P(None, 'space'), may hold values from -6 to 6
- modes: float32 [16, 32], replicated, may hold values from -1 to 1
- legendre: bfloat16 [512, 512, 256], P('space'), may hold values from -0.25 to 0.25
- spectrum: float32 [512, 256], P('space'), may hold values from 0.1 to 1
- truncation: int32 [1], replicated, may hold values from 543 to 702
Outputs:
- covariance_apply: bfloat16 [32, 512, 1536], P(None, 'space')
The draws below stay inside these ranges and needn't reach their ends.
All inputs are finite; a program needn't handle non-finite values.
Results may differ from the reference program's by a relative error of at most 0.014.
Values may be sent and summed in bfloat16 or wider, within the bound.
No kernel may reach another device: no remote copies, remote signals or barrier semaphores. Data moves between devices by JAX's collectives and lax.ppermute only.
A program may use at most 128 MiB of HBM per device.

```python
import math
import jax
import jax.numpy as jnp
from jax import lax

NLEV = 32
NMODE = 16
NLON = 1536
NLAT = 512
M = 512
NDEG = 256
MEMBERS = 32


def block_scale(key, shape, shards, low, largest):
    loudness = 1.0
    for axis_at, parts in shards:
        steps = jax.random.uniform(jax.random.fold_in(jax.random.fold_in(key, 6), axis_at), (parts,), jnp.float32, low / len(shards), largest / len(shards))
        loudness = loudness * jnp.repeat(jnp.exp(steps), shape[axis_at] // parts).reshape((-1,) + (1,) * (len(shape) - 1 - axis_at))
    return loudness


def scatter_about(own_key, shape, deviation, bound, shards=(), kind=jnp.bfloat16):
    loudness = block_scale(own_key, shape, shards, -0.22, 0.18) if shards else 1.0
    values = jax.random.normal(own_key, shape, jnp.float32) * deviation * loudness
    return jnp.minimum(jnp.maximum(values, -bound), bound).astype(kind)


def setup_inputs(seed: int = 0) -> dict:
    key_list = jax.random.split(jax.random.key(seed), 7)
    return {
        "ensemble": scatter_about(key_list[0], (MEMBERS, NLEV, NLAT, NLON), 2.0, 12.0, ((0, 8), (2, 32))),
        "vector": scatter_about(key_list[1], (NLEV, NLAT, NLON), 1.0, 6.0, ((1, 32),)),
        "modes": scatter_about(key_list[2], (NMODE, NLEV), NLEV ** -0.5, 1.0, (), jnp.float32),
        "legendre": scatter_about(key_list[3], (M, NLAT, NDEG), NLAT ** -0.5, 0.25, ((0, 32),)),
        "spectrum": jnp.clip(jnp.exp(math.log(1.0) - 2.3025851 * jax.random.uniform(key_list[4], (M, NDEG), jnp.float32) ** block_scale(key_list[4], (M, NDEG), ((0, 32),), -0.2, 0.2)), 0.1, 1.0),
        "truncation": jax.random.randint(key_list[5], (1,), M - 1 + NDEG // 8, M - 1 + 3 * NDEG // 4).astype(jnp.int32),
    }


def fourier_table(length, wave_count):
    points = jnp.arange(length, dtype=jnp.int32)
    orders = jnp.arange(wave_count, dtype=jnp.int32)
    phases = points[:, None] * orders[None, :] % length
    angles = phases.astype(jnp.float32) * (2.0 * math.pi / length)
    amplitude = math.sqrt(2.0 / length)
    stacked = jnp.stack([jnp.cos(angles), -jnp.sin(angles)], axis=-1) * amplitude
    return stacked.reshape(length, 2 * wave_count).astype(jnp.bfloat16)

def reference(ensemble, vector, modes, legendre, spectrum, truncation):
    fourier = fourier_table(NLON, M)
    wavenumber = jnp.arange(M, dtype=jnp.int32)[:, None] + jnp.arange(NDEG, dtype=jnp.int32)[None, :]
    factor = jnp.where(wavenumber <= truncation[0], spectrum, jnp.zeros_like(spectrum))
    legendre_wide = legendre.astype(jnp.float32)
    vector_wide = vector.astype(jnp.float32)
    highest = lax.Precision.HIGHEST

    def member(running, anomaly):
        product = anomaly.astype(jnp.float32) * vector_wide
        projected = jnp.einsum('jl,lac->jac', modes, product, precision=highest).astype(jnp.bfloat16)
        zonal_parts = jnp.dot(projected.reshape(NMODE * NLAT, NLON), fourier, preferred_element_type=jnp.float32)
        zonal_parts = lax.optimization_barrier(zonal_parts.astype(jnp.bfloat16))
        zonal_wide = zonal_parts.astype(jnp.float32).reshape(NMODE, NLAT, M, 2)
        harmonic = jnp.einsum('jamr,man->jmrn', zonal_wide, legendre_wide)
        weighted = lax.optimization_barrier((harmonic * factor[None, :, None, :]).astype(jnp.bfloat16))
        weighted_wide = weighted.astype(jnp.float32)
        synthesis = jnp.einsum('jmrn,man->jamr', weighted_wide, legendre_wide).astype(jnp.bfloat16)
        spread = jnp.dot(synthesis.reshape(NMODE * NLAT, 2 * M), fourier.T, preferred_element_type=jnp.float32)
        spread = spread.reshape(NMODE, NLAT, NLON)
        lifted = jnp.einsum('jl,jac->lac', modes, spread, precision=highest)
        return (running + anomaly.astype(jnp.float32) * lifted, None)
    start = jnp.zeros((NLEV, NLAT, NLON), jnp.float32)
    summed, _ = lax.scan(member, start, ensemble)
    return (summed / (MEMBERS - 1)).astype(jnp.bfloat16)
```

```python
import math

import jax
import jax.numpy as jnp
import numpy as np
from jax import lax
from jax.experimental import pallas as pl
from jax.experimental.pallas import tpu as pltpu
from jax.sharding import Mesh
from jax.sharding import PartitionSpec as P

NLON = 1536
M = 512
SPACE = ("space_0", "space_1", "space_2")
F32 = jnp.float32
BF16 = jnp.bfloat16
NT = (((1,), (1,)), ((), ()))
TN = (((0,), (0,)), ((), ()))


def angle_tables(block):
    points = np.arange(NLON)[None, :]
    amplitude = math.sqrt(2.0 / NLON)

    def angles(waves):
        return (points * waves[:, None] % NLON) * (2.0 * math.pi / NLON)

    low = angles(np.arange(block))
    high = angles(np.arange(M // block) * block)
    tables = (np.cos(low) * amplitude, np.sin(low) * amplitude, np.cos(high), np.sin(high))
    return [jnp.asarray(t, F32) for t in tables]


def iota2(shape, dim):
    return lax.broadcasted_iota(jnp.int32, shape, dim)


def one_hot(match):
    return jnp.where(match, 1.0, 0.0).astype(BF16)


def forward_kernel(modes_ref, low_c, low_s, high_c, high_s, e_ref, v_ref, z_ref, ft_ref, kp, p, y):
    k = pl.program_id(0)
    members = pl.num_programs(0)
    block = low_c.shape[0]
    modes_n, levels = modes_ref.shape
    rows = kp.shape[0] // modes_n
    fields = p.shape[0] // rows

    @pl.when(k == 0)
    def _():
        ra = one_hot(iota2((rows * modes_n, modes_n), 0) % modes_n == iota2((rows * modes_n, modes_n), 1))
        la = one_hot(iota2((levels, levels * rows), 1) // rows == iota2((levels, levels * rows), 0))
        spread_rows = jnp.dot(ra, modes_ref[...].astype(BF16), preferred_element_type=F32)
        full = jnp.dot(spread_rows.astype(BF16), la, preferred_element_type=F32)
        mask = iota2(kp.shape, 0) // modes_n == iota2(kp.shape, 1) % rows
        kp[...] = jnp.where(mask, full, 0.0).astype(BF16)

        def build(t, carry):
            hc = high_c[pl.ds(t, 1), :]
            hs = high_s[pl.ds(t, 1), :]
            at = pl.multiple_of(t * block, block)
            ft_ref[pl.ds(at, block), :] = (low_c[...] * hc - low_s[...] * hs).astype(BF16)
            ft_ref[pl.ds(M + at, block), :] = -(low_s[...] * hc + low_c[...] * hs).astype(BF16)
            return carry

        lax.fori_loop(0, M // block, build, 0)

    product = e_ref[0] * v_ref[...]
    projected = jnp.dot(kp[...], product, preferred_element_type=F32).astype(BF16)
    for a in range(rows):
        at = pl.multiple_of(a * fields + k * modes_n, modes_n)
        p[pl.ds(at, modes_n), :] = projected[a * modes_n : (a + 1) * modes_n]

    @pl.when(k == members - 1)
    def _():
        lane = iota2((M, 2 * fields), 1)
        for chunk in range(rows // 4):
            wide = 4 * fields
            got = lax.dot_general(
                ft_ref[...], p[chunk * wide : (chunk + 1) * wide, :], NT, preferred_element_type=F32
            )
            for pair in range(2):
                lanes = slice(pair * 2 * fields, (pair + 1) * 2 * fields)
                tc = got[:M, lanes]
                ts = got[M:, lanes]
                a = chunk * 4 + pair * 2
                y[pl.ds(a, M, stride=rows), :] = jnp.where(lane < fields, tc, pltpu.roll(ts, fields, 1))
                y[pl.ds(a + 1, M, stride=rows), :] = jnp.where(lane < fields, pltpu.roll(tc, fields, 1), ts)

        z_ref[...] = y[...].astype(BF16)


def forward(modes, ensemble, vector):
    members, levels, rows, lons = ensemble.shape
    modes_n = modes.shape[0]
    fields = members * modes_n
    low_c, low_s, high_c, high_s = angle_tables(16)
    whole = lambda s: pl.BlockSpec(s, lambda k: (0,) * len(s))
    return pl.pallas_call(
        forward_kernel,
        grid=(members,),
        in_specs=[
            whole(modes.shape),
            whole(low_c.shape),
            whole(low_s.shape),
            whole(high_c.shape),
            whole(high_s.shape),
            pl.BlockSpec((1, levels * rows, lons), lambda k: (k, 0, 0)),
            whole((levels * rows, lons)),
        ],
        out_specs=[whole((M * rows, 2 * fields)), whole((2 * M, lons))],
        out_shape=[
            jax.ShapeDtypeStruct((M * rows, 2 * fields), BF16),
            jax.ShapeDtypeStruct((2 * M, lons), BF16),
        ],
        scratch_shapes=[
            pltpu.VMEM((rows * modes_n, levels * rows), BF16),
            pltpu.VMEM((rows * fields, lons), BF16),
            pltpu.VMEM((M * rows, 2 * fields), F32),
        ],
        compiler_params=pltpu.CompilerParams(vmem_limit_bytes=56 * 2**20),
        name="forward",
    )(
        modes,
        low_c,
        low_s,
        high_c,
        high_s,
        ensemble.reshape(members, levels * rows, lons),
        vector.reshape(levels * rows, lons),
    )


def spectral_kernel(scalars, spectrum_ref, x_ref, l_ref, out_ref, s):
    step = pl.program_id(0)
    sources, per, rows, lanes = x_ref.shape
    waves = per * pl.num_programs(0)
    degrees = l_ref.shape[2]
    for i in range(per):
        m = step * per + i
        x = x_ref[:, i].reshape(sources * rows, lanes)
        harmonic = lax.dot_general(x, l_ref[i], TN, preferred_element_type=F32)
        total = scalars[1] + m + iota2((1, degrees), 1)
        factor = jnp.where(total <= scalars[0], spectrum_ref[pl.ds(m, 1), :], 0.0)
        weighted = (harmonic * factor).astype(BF16)
        back = lax.dot_general(l_ref[i], weighted, NT, preferred_element_type=F32)
        s[pl.ds(m, sources * rows, stride=waves), :] = back

    @pl.when(step == pl.num_programs(0) - 1)
    def _():
        out_ref[...] = s[...].astype(BF16)


def spectral(scalars, spectrum, arrived, legendre):
    sources, waves, rows, lanes = arrived.shape
    lats, degrees = legendre.shape[1:]
    per = 4
    return pl.pallas_call(
        spectral_kernel,
        grid_spec=pltpu.PrefetchScalarGridSpec(
            num_scalar_prefetch=1,
            grid=(waves // per,),
            in_specs=[
                pl.BlockSpec((waves, degrees), lambda i, _: (0, 0)),
                pl.BlockSpec((sources, per, rows, lanes), lambda i, _: (0, i, 0, 0)),
                pl.BlockSpec((per, lats, degrees), lambda i, _: (i, 0, 0)),
            ],
            out_specs=pl.BlockSpec((sources * rows * waves, lanes), lambda i, _: (0, 0)),
            scratch_shapes=[pltpu.VMEM((sources * rows * waves, lanes), F32)],
        ),
        out_shape=jax.ShapeDtypeStruct((sources * rows * waves, lanes), BF16),
        compiler_params=pltpu.CompilerParams(vmem_limit_bytes=40 * 2**20),
        name="spectral",
    )(scalars, spectrum, arrived, legendre)


def backward_kernel(modes_ref, r_ref, ft_ref, e_ref, out_ref, kl, g):
    modes_n, levels = modes_ref.shape
    sources, rows, waves, lanes = r_ref.shape
    members = e_ref.shape[0]
    fields = members * modes_n

    @pl.when(pl.program_id(0) == 0)
    def _():
        la = one_hot(iota2((levels * rows, levels), 0) // rows == iota2((levels * rows, levels), 1))
        ra = one_hot(iota2((modes_n, rows * modes_n), 1) % modes_n == iota2((modes_n, rows * modes_n), 0))
        spread_rows = lax.dot_general(la, modes_ref[...].astype(BF16), NT, preferred_element_type=F32)
        full = jnp.dot(spread_rows.astype(BF16), ra, preferred_element_type=F32)
        mask = iota2(kl.shape, 0) % rows == iota2(kl.shape, 1) // modes_n
        kl[...] = jnp.where(mask, full, 0.0).astype(BF16)
        for a in range(rows):
            flipped = r_ref[:, a].reshape(sources * waves, lanes).T
            for r in range(2):
                for k in range(members):
                    at = r * fields + k * modes_n
                    to = k * rows * modes_n + a * modes_n
                    g[to : to + modes_n, r * M : (r + 1) * M] = flipped[at : at + modes_n]

    spread = jnp.dot(g[...], ft_ref[...], preferred_element_type=F32).astype(BF16)
    share = rows * modes_n
    total = None
    for k in range(members):
        lifted = jnp.dot(kl[...], spread[k * share : (k + 1) * share], preferred_element_type=F32)
        term = e_ref[k].astype(F32) * lifted
        total = term if total is None else total + term
    out_ref[...] = total.astype(BF16)


def backward(modes, returned, fourier, ensemble):
    members, levels, rows, lons = ensemble.shape
    modes_n = modes.shape[0]
    chunk = 256
    return pl.pallas_call(
        backward_kernel,
        grid=(lons // chunk,),
        in_specs=[
            pl.BlockSpec(modes.shape, lambda i: (0, 0)),
            pl.BlockSpec(returned.shape, lambda i: (0, 0, 0, 0)),
            pl.BlockSpec((2 * M, chunk), lambda i: (0, i)),
            pl.BlockSpec((members, levels * rows, chunk), lambda i: (0, 0, i)),
        ],
        out_specs=pl.BlockSpec((levels * rows, chunk), lambda i: (0, i)),
        out_shape=jax.ShapeDtypeStruct((levels * rows, lons), BF16),
        scratch_shapes=[
            pltpu.VMEM((levels * rows, rows * modes_n), BF16),
            pltpu.VMEM((members * rows * modes_n, 2 * M), BF16),
        ],
        compiler_params=pltpu.CompilerParams(vmem_limit_bytes=48 * 2**20),
        name="backward",
    )(modes, returned, fourier, ensemble.reshape(members, levels * rows, lons))


def swap(blocks, axes):
    return lax.all_to_all(blocks, axes, 0, 0, tiled=True)


def on_device(ensemble, vector, modes, legendre, spectrum, truncation):
    members, levels, rows, lons = ensemble.shape
    waves = legendre.shape[0]
    sources = lax.axis_size(SPACE)
    groups = lax.axis_size("mem")
    lanes = 2 * members * modes.shape[0]
    zonal, fourier = forward(modes, ensemble, vector)
    arrived = swap(zonal.reshape(sources, waves, rows, lanes), SPACE)
    first_wave = lax.axis_index(SPACE) * waves
    scalars = jnp.concatenate([truncation, first_wave.astype(jnp.int32)[None]])
    synthesis = spectral(scalars, spectrum, arrived, legendre)
    returned = swap(synthesis.reshape(sources, rows, waves, lanes), SPACE)
    partial_value = backward(modes, returned, fourier, ensemble)
    blocks = swap(partial_value.reshape(groups, levels // groups, rows, lons), "mem")
    share = jnp.sum(blocks.astype(F32), axis=0)
    rounded = (share / (members * groups - 1)).astype(BF16)
    gathered = swap(jnp.broadcast_to(rounded[None], (groups, *rounded.shape)), "mem")
    return gathered.reshape(levels, rows, lons)


def solution(mesh):
    torus = Mesh(
        mesh.devices.reshape(4, 4, 2, mesh.shape["mem"]), ("space_0", "space_1", "space_2", "mem")
    )
    in_specs = (
        P("mem", None, SPACE, None),
        P(None, SPACE, None),
        P(),
        P(SPACE, None, None),
        P(SPACE, None),
        P(),
    )
    out_specs = P(None, SPACE, None)
    return jax.shard_map(
        on_device, mesh=torus, in_specs=in_specs, out_specs=out_specs, check_vma=False
    )
```

```python
import functools
import math

import jax
import jax.numpy as jnp
import numpy as np
from jax import lax
from jax.experimental import pallas as pl
from jax.experimental.pallas import tpu as pltpu
from jax.sharding import Mesh
from jax.sharding import PartitionSpec as P


NLON = 1536
M = 512
SPACE = ("space_0", "space_1", "space_2")
F32 = jnp.float32
BF16 = jnp.bfloat16
NT = (((1,), (1,)), ((), ()))
TN = (((0,), (0,)), ((), ()))


def angle_tables(block):
    points = np.arange(NLON)[None, :]
    amplitude = math.sqrt(2.0 / NLON)

    def angles(waves):
        return (points * waves[:, None] % NLON) * (2.0 * math.pi / NLON)

    low = angles(np.arange(block))
    high = angles(np.arange(M // block) * block)
    tables = (np.cos(low) * amplitude, np.sin(low) * amplitude, np.cos(high), np.sin(high))
    return [jnp.asarray(t, F32) for t in tables]


def iota2(shape, dim):
    return lax.broadcasted_iota(jnp.int32, shape, dim)


def one_hot(match):
    return jnp.where(match, 1.0, 0.0).astype(BF16)


def build_table(ft_ref, low_c, low_s, high_c, high_s):
    block = low_c.shape[0]

    def build(t, carry):
        hc = high_c[pl.ds(t, 1), :]
        hs = high_s[pl.ds(t, 1), :]
        at = pl.multiple_of(t * block, block)
        ft_ref[pl.ds(at, block), :] = (low_c[...] * hc - low_s[...] * hs).astype(BF16)
        ft_ref[pl.ds(M + at, block), :] = -(low_s[...] * hc + low_c[...] * hs).astype(BF16)
        return carry

    lax.fori_loop(0, M // block, build, 0)


def forward_kernel(modes_ref, low_c, low_s, high_c, high_s, e_ref, v_ref, z_ref, ft_ref, kp, p, y):
    k = pl.program_id(0)
    members = pl.num_programs(0)
    modes_n, levels = modes_ref.shape
    rows = kp.shape[0] // modes_n
    fields = p.shape[0] // rows

    @pl.when(k == 0)
    def _():
        ra = one_hot(iota2((rows * modes_n, modes_n), 0) % modes_n == iota2((rows * modes_n, modes_n), 1))
        la = one_hot(iota2((levels, levels * rows), 1) // rows == iota2((levels, levels * rows), 0))
        spread_rows = jnp.dot(ra, modes_ref[...].astype(BF16), preferred_element_type=F32)
        full = jnp.dot(spread_rows.astype(BF16), la, preferred_element_type=F32)
        mask = iota2(kp.shape, 0) // modes_n == iota2(kp.shape, 1) % rows
        kp[...] = jnp.where(mask, full, 0.0).astype(BF16)

        build_table(ft_ref, low_c, low_s, high_c, high_s)

    product = e_ref[0] * v_ref[...]
    projected = jnp.dot(kp[...], product, preferred_element_type=F32).astype(BF16)
    for a in range(rows):
        at = pl.multiple_of(a * fields + k * modes_n, modes_n)
        p[pl.ds(at, modes_n), :] = projected[a * modes_n : (a + 1) * modes_n]

    @pl.when(k == members - 1)
    def _():
        lane = iota2((M, 2 * fields), 1)
        for chunk in range(rows // 4):
            wide = 4 * fields
            got = lax.dot_general(
                ft_ref[...], p[chunk * wide : (chunk + 1) * wide, :], NT, preferred_element_type=F32
            )
            for pair in range(2):
                lanes = slice(pair * 2 * fields, (pair + 1) * 2 * fields)
                tc = got[:M, lanes]
                ts = got[M:, lanes]
                a = chunk * 4 + pair * 2
                y[pl.ds(a, M, stride=rows), :] = jnp.where(lane < fields, tc, pltpu.roll(ts, fields, 1))
                y[pl.ds(a + 1, M, stride=rows), :] = jnp.where(lane < fields, pltpu.roll(tc, fields, 1), ts)

        z_ref[...] = y[...].astype(BF16)


def forward(modes, ensemble, vector):
    members, levels, rows, lons = ensemble.shape
    modes_n = modes.shape[0]
    fields = members * modes_n
    low_c, low_s, high_c, high_s = angle_tables(16)
    whole = lambda s: pl.BlockSpec(s, lambda k: (0,) * len(s))
    return pl.pallas_call(
        forward_kernel,
        grid=(members,),
        in_specs=[
            whole(modes.shape),
            whole(low_c.shape),
            whole(low_s.shape),
            whole(high_c.shape),
            whole(high_s.shape),
            pl.BlockSpec((1, levels * rows, lons), lambda k: (k, 0, 0)),
            whole((levels * rows, lons)),
        ],
        out_specs=whole((M * rows, 2 * fields)),
        out_shape=jax.ShapeDtypeStruct((M * rows, 2 * fields), BF16),
        scratch_shapes=[
            pltpu.VMEM((2 * M, lons), BF16),
            pltpu.VMEM((rows * modes_n, levels * rows), BF16),
            pltpu.VMEM((rows * fields, lons), BF16),
            pltpu.VMEM((M * rows, 2 * fields), F32),
        ],
        compiler_params=pltpu.CompilerParams(vmem_limit_bytes=62 * 2**20),
        name="forward",
    )(
        modes,
        low_c,
        low_s,
        high_c,
        high_s,
        ensemble.reshape(members, levels * rows, lons),
        vector.reshape(levels * rows, lons),
    )


def divide_kernel(scalars, low_c, low_s, high_c, high_s, e_ref, *rest, rows):
    *out_refs, ft_ref, perm = rest
    parts = len(out_refs)
    share = out_refs[0].shape[1]
    own = scalars[2]

    @pl.when(pl.program_id(0) == 0)
    def _():
        build_table(ft_ref, low_c, low_s, high_c, high_s)
        row = iota2(perm.shape, 0)
        col = iota2(perm.shape, 1)
        per = rows // parts
        part = (own + row // share) % parts
        level = row % share // per
        lat = part * per + row % per
        perm[...] = one_hot(col == level * rows + lat)

    moved = jnp.dot(perm[...], e_ref[0], preferred_element_type=F32).astype(BF16)
    for d, out_ref in enumerate(out_refs):
        out_ref[0] = moved[d * share : (d + 1) * share]


def divide(scalars, ensemble, parts):
    members, levels, rows, lons = ensemble.shape
    share = levels * rows // parts
    tables = angle_tables(16)
    return pl.pallas_call(
        functools.partial(divide_kernel, rows=rows),
        grid_spec=pltpu.PrefetchScalarGridSpec(
            num_scalar_prefetch=1,
            grid=(members,),
            in_specs=[pl.BlockSpec(t.shape, lambda k, _: (0, 0)) for t in tables]
            + [pl.BlockSpec((1, levels * rows, lons), lambda k, _: (k, 0, 0))],
            out_specs=[pl.BlockSpec((1, share, lons), lambda k, _: (k, 0, 0))] * parts
            + [pl.BlockSpec((2 * M, lons), lambda k, _: (0, 0))],
            scratch_shapes=[pltpu.VMEM((levels * rows, levels * rows), BF16)],
        ),
        out_shape=[jax.ShapeDtypeStruct((members, share, lons), BF16)] * parts
        + [jax.ShapeDtypeStruct((2 * M, lons), BF16)],
        compiler_params=pltpu.CompilerParams(vmem_limit_bytes=62 * 2**20),
        cost_estimate=pl.CostEstimate(flops=10**10, bytes_accessed=2 * 10**7, transcendentals=0),
        name="divide",
    )(scalars, *tables, ensemble.reshape(members, levels * rows, lons))


def spectral_kernel(scalars, spectrum_ref, x_ref, l_hbm, out_ref, s, l_all, arrive):
    step = pl.program_id(0)
    sources, per, rows, lanes = x_ref.shape
    waves = l_all.shape[0]
    degrees = l_all.shape[2]

    def load(at):
        part = pl.ds(at * per, per)
        return pltpu.make_async_copy(l_hbm.at[part], l_all.at[part], arrive.at[at])

    @pl.when(step == 0)
    def _():
        for at in range(waves // per):
            load(at).start()

    load(step).wait()
    for i in range(per):
        m = step * per + i
        x = x_ref[:, i].reshape(sources * rows, lanes)
        harmonic = lax.dot_general(x, l_all[m], TN, preferred_element_type=F32)
        total = scalars[1] + m + iota2((1, degrees), 1)
        factor = jnp.where(total <= scalars[0], spectrum_ref[pl.ds(m, 1), :], 0.0)
        weighted = (harmonic * factor).astype(BF16)
        back = lax.dot_general(l_all[m], weighted, NT, preferred_element_type=F32)
        s[pl.ds(m, sources * rows, stride=waves), :] = back

    @pl.when(step == pl.num_programs(0) - 1)
    def _():
        out_ref[...] = s[...].astype(BF16)


def spectral(scalars, spectrum, arrived, legendre):
    sources, waves, rows, lanes = arrived.shape
    lats, degrees = legendre.shape[1:]
    per = 4
    return pl.pallas_call(
        spectral_kernel,
        grid_spec=pltpu.PrefetchScalarGridSpec(
            num_scalar_prefetch=1,
            grid=(waves // per,),
            in_specs=[
                pl.BlockSpec((waves, degrees), lambda i, _: (0, 0)),
                pl.BlockSpec((sources, per, rows, lanes), lambda i, _: (0, i, 0, 0)),
                pl.BlockSpec(memory_space=pltpu.MemorySpace.HBM),
            ],
            out_specs=pl.BlockSpec((sources * rows * waves, lanes), lambda i, _: (0, 0)),
            scratch_shapes=[
                pltpu.VMEM((sources * rows * waves, lanes), F32),
                pltpu.VMEM((waves, lats, degrees), BF16),
                pltpu.SemaphoreType.DMA((waves // per,)),
            ],
        ),
        out_shape=jax.ShapeDtypeStruct((sources * rows * waves, lanes), BF16),
        compiler_params=pltpu.CompilerParams(vmem_limit_bytes=62 * 2**20),
        name="spectral",
    )(scalars, spectrum, arrived, legendre)


def backward_kernel(scalars, modes_ref, r_ref, ft_ref, *rest):
    *e_refs, out_ref, kl, g = rest
    modes_n, levels = modes_ref.shape
    sources, parts, rows, waves, lanes = r_ref.shape
    members = e_refs[0].shape[0]
    fields = members * modes_n
    share = levels * rows
    columns = rows * modes_n

    @pl.when(pl.program_id(0) == 0)
    def _():
        height, width = kl.shape
        la = one_hot(iota2((height, levels), 0) % share // rows == iota2((height, levels), 1))
        ra = one_hot(iota2((modes_n, width), 1) % modes_n == iota2((modes_n, width), 0))
        spread_rows = lax.dot_general(la, modes_ref[...].astype(BF16), NT, preferred_element_type=F32)
        full = jnp.dot(spread_rows.astype(BF16), ra, preferred_element_type=F32)
        row = iota2(kl.shape, 0)
        col = iota2(kl.shape, 1)
        mask = (row // share == col // columns) & (row % rows == col % columns // modes_n)
        kl[...] = jnp.where(mask, full, 0.0).astype(BF16)
        for d in range(parts):
            source = (scalars[2] + parts - d) % parts
            for a in range(rows):
                flipped = r_ref[:, source, a].reshape(sources * waves, lanes).T
                for r in range(2):
                    for k in range(members):
                        at = r * fields + k * modes_n
                        to = (d * members + k) * columns + a * modes_n
                        g[to : to + modes_n, r * M : (r + 1) * M] = flipped[at : at + modes_n]

    spread = jnp.dot(g[...], ft_ref[...], preferred_element_type=F32).astype(BF16)
    group = members * columns
    total = None
    for d in range(parts):
        lifted = jnp.dot(kl[...], spread[d * group : (d + 1) * group], preferred_element_type=F32)
        for k in range(members):
            term = e_refs[d][k].astype(F32) * lifted[k * share : (k + 1) * share]
            total = term if total is None else total + term
    out_ref[...] = total.astype(BF16)


def backward(scalars, modes, returned, fourier, pieces):
    _, parts, rows, _, _ = returned.shape
    members, share, lons = pieces[0].shape
    modes_n = modes.shape[0]
    chunk = 256
    columns = members * rows * modes_n
    return pl.pallas_call(
        backward_kernel,
        grid_spec=pltpu.PrefetchScalarGridSpec(
            num_scalar_prefetch=1,
            grid=(lons // chunk,),
            in_specs=[
                pl.BlockSpec(modes.shape, lambda i, _: (0, 0)),
                pl.BlockSpec(returned.shape, lambda i, _: (0, 0, 0, 0, 0)),
                pl.BlockSpec((2 * M, chunk), lambda i, _: (0, i)),
            ]
            + [pl.BlockSpec((members, share, chunk), lambda i, _: (0, 0, i))] * parts,
            out_specs=pl.BlockSpec((share, chunk), lambda i, _: (0, i)),
            scratch_shapes=[
                pltpu.VMEM((members * share, columns), BF16),
                pltpu.VMEM((parts * columns, 2 * M), BF16),
            ],
        ),
        out_shape=jax.ShapeDtypeStruct((share, lons), BF16),
        compiler_params=pltpu.CompilerParams(vmem_limit_bytes=62 * 2**20),
        name="backward",
    )(scalars, modes, returned, fourier, *pieces)


def place_kernel(x_ref, out_ref, perm, *, levels):
    parts, halves, share, chunk = x_ref.shape
    height = perm.shape[0]

    @pl.when(pl.program_id(0) == 0)
    def _():
        rows = height // levels
        row = iota2(perm.shape, 0)
        level = row // rows
        lat = row % rows
        per = rows // parts
        half = levels // halves
        wanted = (lat // per * halves + level // half) * share + level % half * per + lat % per
        perm[...] = one_hot(iota2(perm.shape, 1) == wanted)

    x = x_ref[...].reshape(height, chunk)
    out_ref[...] = jnp.dot(perm[...], x, preferred_element_type=F32).astype(BF16)


def place(gathered, levels):
    parts, halves, share, lons = gathered.shape
    chunk = 256
    height = parts * halves * share
    return pl.pallas_call(
        functools.partial(place_kernel, levels=levels),
        grid=(lons // chunk,),
        in_specs=[pl.BlockSpec((parts, halves, share, chunk), lambda i: (0, 0, 0, i))],
        out_specs=pl.BlockSpec((height, chunk), lambda i: (0, i)),
        out_shape=jax.ShapeDtypeStruct((height, lons), BF16),
        scratch_shapes=[pltpu.VMEM((height, height), BF16)],
        compiler_params=pltpu.CompilerParams(vmem_limit_bytes=62 * 2**20),
        name="place",
    )(gathered)


def swap(blocks, axes):
    return lax.all_to_all(blocks, axes, 0, 0, tiled=True)


def on_device(ensemble, vector, modes, legendre, spectrum, truncation):
    members, levels, rows, lons = ensemble.shape
    waves = legendre.shape[0]
    sources = lax.axis_size(SPACE)
    parts = lax.axis_size("mem_y")
    halves = lax.axis_size("mem_z")
    lanes = 2 * members * modes.shape[0]
    quarter = rows // parts
    first_wave = lax.axis_index(SPACE) * waves
    scalars = jnp.stack([truncation[0], first_wave.astype(jnp.int32), lax.axis_index("mem_y").astype(jnp.int32)])
    zonal = forward(modes, ensemble, vector)
    arrived = swap(zonal.reshape(sources, waves, rows, lanes), SPACE)
    held, _ = lax.optimization_barrier((ensemble, zonal))
    *pieces, fourier = divide(scalars, held, parts)
    for d in range(1, parts):
        pieces[d] = lax.ppermute(pieces[d], "mem_y", [(i, (i + d) % parts) for i in range(parts)])
    synthesis = spectral(scalars, spectrum, arrived, legendre)
    returned = swap(synthesis.reshape(sources * parts, quarter, waves, lanes), SPACE + ("mem_y",))
    partial_value = backward(scalars, modes, returned.reshape(sources, parts, quarter, waves, lanes), fourier, pieces)
    blocks = swap(partial_value.reshape(halves, -1, lons), "mem_z")
    share = jnp.sum(blocks.astype(F32), axis=0)
    rounded = (share / (members * parts * halves - 1)).astype(BF16)
    everyone = jnp.broadcast_to(rounded[None], (parts * halves, *rounded.shape))
    gathered = swap(everyone, ("mem_y", "mem_z"))
    return place(gathered.reshape(parts, halves, -1, lons), levels).reshape(levels, rows, lons)


def solution(mesh):
    torus = Mesh(
        mesh.devices.reshape(4, 4, 2, 4, 2), ("space_0", "space_1", "space_2", "mem_y", "mem_z")
    )
    in_specs = (
        P(("mem_y", "mem_z"), None, SPACE, None),
        P(None, SPACE, None),
        P(),
        P(SPACE, None, None),
        P(SPACE, None),
        P(),
    )
    out_specs = P(None, SPACE, None)
    return jax.shard_map(on_device, mesh=torus, in_specs=in_specs, out_specs=out_specs, check_vma=False)
```

```python
import functools
import math

import jax
import jax.numpy as jnp
import numpy as np
from jax import lax
from jax.experimental import pallas as pl
from jax.experimental.pallas import tpu as pltpu
from jax.sharding import Mesh
from jax.sharding import PartitionSpec as P


NLON = 1536
M = 512
SPACE = ("space_0", "space_1", "space_2")
F32 = jnp.float32
BF16 = jnp.bfloat16
NT = (((1,), (1,)), ((), ()))
TN = (((0,), (0,)), ((), ()))


def angle_tables(block):
    points = np.arange(NLON)[None, :]
    amplitude = math.sqrt(2.0 / NLON)

    def angles(waves):
        return (points * waves[:, None] % NLON) * (2.0 * math.pi / NLON)

    low = angles(np.arange(block))
    high = angles(np.arange(M // block) * block)
    tables = (np.cos(low) * amplitude, np.sin(low) * amplitude, np.cos(high), np.sin(high))
    return [jnp.asarray(t, F32) for t in tables]


def iota2(shape, dim):
    return lax.broadcasted_iota(jnp.int32, shape, dim)


def over(value, size):
    assert size & (size - 1) == 0
    return value >> (size.bit_length() - 1)


def rest_of(value, size):
    assert size & (size - 1) == 0
    return value & (size - 1)


def one_hot(match):
    return jnp.where(match, 1.0, 0.0).astype(BF16)


def build_table(ft_ref, low_c, low_s, high_c, high_s):
    block = low_c.shape[0]

    def build(t, carry):
        hc = high_c[pl.ds(t, 1), :]
        hs = high_s[pl.ds(t, 1), :]
        at = pl.multiple_of(t * block, block)
        ft_ref[pl.ds(at, block), :] = (low_c[...] * hc - low_s[...] * hs).astype(BF16)
        ft_ref[pl.ds(M + at, block), :] = -(low_s[...] * hc + low_c[...] * hs).astype(BF16)
        return carry

    lax.fori_loop(0, M // block, build, 0)


def forward_kernel(modes_ref, low_c, low_s, high_c, high_s, e_hbm, v_hbm, z_hbm, ft, kp, p, y, e, v, z, arrive, leave):
    modes_n, levels = modes_ref.shape
    members = e.shape[0]
    rows = kp.shape[0] // modes_n
    fields = p.shape[0] // rows
    loads = [pltpu.make_async_copy(v_hbm, v, arrive.at[members])]
    for k in range(members):
        loads.append(pltpu.make_async_copy(e_hbm.at[k], e.at[k], arrive.at[k]))
    for load in loads:
        load.start()

    build_table(ft, low_c, low_s, high_c, high_s)
    ra = one_hot(rest_of(iota2((rows * modes_n, modes_n), 0), modes_n) == iota2((rows * modes_n, modes_n), 1))
    la = one_hot(over(iota2((levels, levels * rows), 1), rows) == iota2((levels, levels * rows), 0))
    spread_rows = jnp.dot(ra, modes_ref[...].astype(BF16), preferred_element_type=F32)
    full = jnp.dot(spread_rows.astype(BF16), la, preferred_element_type=F32)
    mask = over(iota2(kp.shape, 0), modes_n) == rest_of(iota2(kp.shape, 1), rows)
    kp[...] = jnp.where(mask, full, 0.0).astype(BF16)

    loads[0].wait()
    for k in range(members):
        loads[1 + k].wait()
        projected = jnp.dot(kp[...], e[k] * v[...], preferred_element_type=F32).astype(BF16)
        for a in range(rows):
            at = a * fields + k * modes_n
            p[at : at + modes_n, :] = projected[a * modes_n : (a + 1) * modes_n]

    lane = iota2((M, 2 * fields), 1)
    wide = 4 * fields
    for chunk in range(rows // 4):
        got = lax.dot_general(
            ft[...], p[chunk * wide : (chunk + 1) * wide, :], NT, preferred_element_type=F32
        )
        for pair in range(2):
            lanes = slice(pair * 2 * fields, (pair + 1) * 2 * fields)
            tc = got[:M, lanes]
            ts = got[M:, lanes]
            a = chunk * 4 + pair * 2
            y[pl.ds(a, M, stride=rows), :] = jnp.where(lane < fields, tc, pltpu.roll(ts, fields, 1))
            y[pl.ds(a + 1, M, stride=rows), :] = jnp.where(lane < fields, pltpu.roll(tc, fields, 1), ts)

    stores = []
    count = leave.shape[0]
    size = z.shape[0] // count
    for i in range(count):
        part = pl.ds(i * size, size)
        z[part, :] = y[part, :].astype(BF16)
        stores.append(pltpu.make_async_copy(z.at[part], z_hbm.at[part], leave.at[i]))
        stores[i].start()
    for store in stores:
        store.wait()


def forward(modes, ensemble, vector):
    members, levels, rows, lons = ensemble.shape
    modes_n = modes.shape[0]
    fields = members * modes_n
    tables = angle_tables(16)
    whole = pl.BlockSpec(memory_space=pltpu.MemorySpace.VMEM)
    outside = pl.BlockSpec(memory_space=pltpu.MemorySpace.HBM)
    return pl.pallas_call(
        forward_kernel,
        in_specs=[whole] * 5 + [outside] * 2,
        out_specs=outside,
        out_shape=jax.ShapeDtypeStruct((M * rows, 2 * fields), BF16),
        scratch_shapes=[
            pltpu.VMEM((2 * M, lons), BF16),
            pltpu.VMEM((rows * modes_n, levels * rows), BF16),
            pltpu.VMEM((rows * fields, lons), BF16),
            pltpu.VMEM((M * rows, 2 * fields), F32),
            pltpu.VMEM((members, levels * rows, lons), BF16),
            pltpu.VMEM((levels * rows, lons), BF16),
            pltpu.VMEM((M * rows, 2 * fields), BF16),
            pltpu.SemaphoreType.DMA((members + 1,)),
            pltpu.SemaphoreType.DMA((8,)),
        ],
        compiler_params=pltpu.CompilerParams(vmem_limit_bytes=62 * 2**20),
        name="forward",
    )(
        modes,
        *tables,
        ensemble.reshape(members, levels * rows, lons),
        vector.reshape(levels * rows, lons),
    )


def divide_kernel(scalars, modes_ref, low_c, low_s, high_c, high_s, e_ref, *rest, rows, halves):
    *out_refs, ft_ref, kl, order, perm = rest
    parts = len(out_refs)
    share = out_refs[0].shape[1]
    modes_n, levels = modes_ref.shape
    per = rows // parts
    columns = per * modes_n

    @pl.when(pl.program_id(0) == 0)
    def _():
        build_table(ft_ref, low_c, low_s, high_c, high_s)
        row = iota2(perm.shape, 0)
        col = iota2(perm.shape, 1)
        part = rest_of(scalars[2] + over(row, share), parts)
        level = over(rest_of(row, share), per)
        perm[...] = one_hot(col == level * rows + part * per + rest_of(row, per))
        level = over(row, rows)
        lat = rest_of(row, rows)
        half = levels // halves
        source = over(lat, per) * halves + over(level, half)
        order[...] = one_hot(col == source * (half * per) + rest_of(level, half) * per + rest_of(lat, per))
        height, width = kl.shape
        la = one_hot(over(rest_of(iota2((height, levels), 0), share), per) == iota2((height, levels), 1))
        ra = one_hot(rest_of(iota2((modes_n, width), 1), modes_n) == iota2((modes_n, width), 0))
        spread_rows = lax.dot_general(la, modes_ref[...].astype(BF16), NT, preferred_element_type=F32)
        full = jnp.dot(spread_rows.astype(BF16), ra, preferred_element_type=F32)
        row = iota2(kl.shape, 0)
        col = iota2(kl.shape, 1)
        mask = (over(row, share) == over(col, columns)) & (
            rest_of(row, per) == over(rest_of(col, columns), modes_n)
        )
        kl[...] = jnp.where(mask, full, 0.0).astype(BF16)

    moved = jnp.dot(perm[...], e_ref[0], preferred_element_type=F32).astype(BF16)
    for d, out_ref in enumerate(out_refs):
        out_ref[0] = moved[d * share : (d + 1) * share]


def divide(scalars, modes, ensemble, parts, halves):
    members, levels, rows, lons = ensemble.shape
    height = levels * rows
    share = height // parts
    columns = members * rows // parts * modes.shape[0]
    tables = angle_tables(16)
    fixed = lambda shape: pl.BlockSpec(shape, lambda k, _: (0, 0))
    return pl.pallas_call(
        functools.partial(divide_kernel, rows=rows, halves=halves),
        grid_spec=pltpu.PrefetchScalarGridSpec(
            num_scalar_prefetch=1,
            grid=(members,),
            in_specs=[fixed(t.shape) for t in (modes, *tables)]
            + [pl.BlockSpec((1, height, lons), lambda k, _: (k, 0, 0))],
            out_specs=[pl.BlockSpec((1, share, lons), lambda k, _: (k, 0, 0))] * parts
            + [fixed((2 * M, lons)), fixed((members * share, columns)), fixed((height, height))],
            scratch_shapes=[pltpu.VMEM((height, height), BF16)],
        ),
        out_shape=[jax.ShapeDtypeStruct((members, share, lons), BF16)] * parts
        + [
            jax.ShapeDtypeStruct((2 * M, lons), BF16),
            jax.ShapeDtypeStruct((members * share, columns), BF16),
            jax.ShapeDtypeStruct((height, height), BF16),
        ],
        compiler_params=pltpu.CompilerParams(vmem_limit_bytes=62 * 2**20),
        cost_estimate=pl.CostEstimate(flops=10**10, bytes_accessed=2 * 10**7, transcendentals=0),
        name="divide",
    )(scalars, modes, *tables, ensemble.reshape(members, height, lons))


def spectral_kernel(scalars, spectrum_ref, x_ref, l_hbm, out_ref, s, l_all, arrive):
    step = pl.program_id(0)
    sources, per, rows, lanes = x_ref.shape
    waves = l_all.shape[0]
    degrees = l_all.shape[2]

    def load(at):
        part = pl.ds(at * per, per)
        return pltpu.make_async_copy(l_hbm.at[part], l_all.at[part], arrive.at[at])

    @pl.when(step == 0)
    def _():
        for at in range(waves // per):
            load(at).start()

    load(step).wait()
    for i in range(per):
        m = step * per + i
        x = x_ref[:, i].reshape(sources * rows, lanes)
        harmonic = lax.dot_general(x, l_all[m], TN, preferred_element_type=F32)
        total = scalars[1] + m + iota2((1, degrees), 1)
        factor = jnp.where(total <= scalars[0], spectrum_ref[pl.ds(m, 1), :], 0.0)
        weighted = (harmonic * factor).astype(BF16)
        back = lax.dot_general(l_all[m], weighted, NT, preferred_element_type=F32)
        s[pl.ds(m, sources * rows, stride=waves), :] = back

    @pl.when(step == pl.num_programs(0) - 1)
    def _():
        out_ref[...] = s[...].astype(BF16)


def spectral(scalars, spectrum, arrived, legendre):
    sources, waves, rows, lanes = arrived.shape
    lats, degrees = legendre.shape[1:]
    per = 4
    return pl.pallas_call(
        spectral_kernel,
        grid_spec=pltpu.PrefetchScalarGridSpec(
            num_scalar_prefetch=1,
            grid=(waves // per,),
            in_specs=[
                pl.BlockSpec((waves, degrees), lambda i, _: (0, 0)),
                pl.BlockSpec((sources, per, rows, lanes), lambda i, _: (0, i, 0, 0)),
                pl.BlockSpec(memory_space=pltpu.MemorySpace.HBM),
            ],
            out_specs=pl.BlockSpec((sources * rows * waves, lanes), lambda i, _: (0, 0)),
            scratch_shapes=[
                pltpu.VMEM((sources * rows * waves, lanes), F32),
                pltpu.VMEM((waves, lats, degrees), BF16),
                pltpu.SemaphoreType.DMA((waves // per,)),
            ],
        ),
        out_shape=jax.ShapeDtypeStruct((sources * rows * waves, lanes), BF16),
        compiler_params=pltpu.CompilerParams(vmem_limit_bytes=50 * 2**20),
        name="spectral",
    )(scalars, spectrum, arrived, legendre)


def backward_kernel(scalars, kl_ref, r_ref, ft_ref, *rest):
    *e_refs, kept_ref, sent_ref, g, sums = rest
    sources, parts, rows, waves, lanes = r_ref.shape
    members, share = e_refs[0].shape[:2]
    fields = lanes // 2
    modes_n = fields // members
    columns = rows * modes_n

    @pl.when(pl.program_id(0) == 0)
    def _():
        for d in range(parts):
            source = rest_of(scalars[2] + parts - d, parts)
            for a in range(rows):
                flipped = r_ref[:, source, a].reshape(sources * waves, lanes).T
                for r in range(2):
                    for k in range(members):
                        at = r * fields + k * modes_n
                        to = (d * members + k) * columns + a * modes_n
                        g[to : to + modes_n, r * M : (r + 1) * M] = flipped[at : at + modes_n]

    spread = jnp.dot(g[...], ft_ref[...], preferred_element_type=F32).astype(BF16)
    group = members * columns
    total = None
    for d in range(parts):
        lifted = jnp.dot(kl_ref[...], spread[d * group : (d + 1) * group], preferred_element_type=F32)
        for k in range(members):
            term = e_refs[d][k].astype(F32) * lifted[k * share : (k + 1) * share]
            total = term if total is None else total + term
    sums[...] = total.astype(BF16)
    half = kept_ref.shape[0]
    at = scalars[3] * half
    kept_ref[...] = sums[pl.ds(pl.multiple_of(at, half), half), :]
    sent_ref[...] = sums[pl.ds(pl.multiple_of(half - at, half), half), :]


def backward(scalars, lift, returned, fourier, pieces, halves):
    _, parts, _, _, _ = returned.shape
    members, share, lons = pieces[0].shape
    chunk = 256
    half = share // halves
    return pl.pallas_call(
        backward_kernel,
        grid_spec=pltpu.PrefetchScalarGridSpec(
            num_scalar_prefetch=1,
            grid=(lons // chunk,),
            in_specs=[
                pl.BlockSpec(lift.shape, lambda i, _: (0, 0)),
                pl.BlockSpec(returned.shape, lambda i, _: (0, 0, 0, 0, 0)),
                pl.BlockSpec((2 * M, chunk), lambda i, _: (0, i)),
            ]
            + [pl.BlockSpec((members, share, chunk), lambda i, _: (0, 0, i))] * parts,
            out_specs=[pl.BlockSpec((half, chunk), lambda i, _: (0, i))] * halves,
            scratch_shapes=[
                pltpu.VMEM((parts * lift.shape[1], 2 * M), BF16),
                pltpu.VMEM((share, chunk), BF16),
            ],
        ),
        out_shape=[jax.ShapeDtypeStruct((half, lons), BF16)] * halves,
        compiler_params=pltpu.CompilerParams(vmem_limit_bytes=50 * 2**20),
        name="backward",
    )(scalars, lift, returned, fourier, *pieces)


def place_kernel(order_ref, x_ref, out_ref):
    out_ref[...] = jnp.dot(order_ref[...], x_ref[...], preferred_element_type=F32).astype(BF16)


def place(order, gathered):
    height, lons = gathered.shape
    chunk = 512
    return pl.pallas_call(
        place_kernel,
        grid=(lons // chunk,),
        in_specs=[
            pl.BlockSpec(order.shape, lambda i: (0, 0)),
            pl.BlockSpec((height, chunk), lambda i: (0, i)),
        ],
        out_specs=pl.BlockSpec((height, chunk), lambda i: (0, i)),
        out_shape=jax.ShapeDtypeStruct((height, lons), BF16),
        compiler_params=pltpu.CompilerParams(vmem_limit_bytes=16 * 2**20),
        name="place",
    )(order, gathered)


def swap(blocks, axes):
    return lax.all_to_all(blocks, axes, 0, 0, tiled=True)


def on_device(ensemble, vector, modes, legendre, spectrum, truncation):
    members, levels, rows, lons = ensemble.shape
    waves = legendre.shape[0]
    sources = lax.axis_size(SPACE)
    parts = lax.axis_size("mem_y")
    halves = lax.axis_size("mem_z")
    lanes = 2 * members * modes.shape[0]
    quarter = rows // parts
    first_wave = lax.axis_index(SPACE) * waves
    places = [first_wave, lax.axis_index("mem_y"), lax.axis_index("mem_z")]
    scalars = jnp.stack([truncation[0], *[i.astype(jnp.int32) for i in places]])
    zonal = forward(modes, ensemble, vector)
    arrived = swap(zonal.reshape(sources, waves, rows, lanes), SPACE)
    held, _ = lax.optimization_barrier((ensemble, zonal))
    *pieces, fourier, lift, order = divide(scalars, modes, held, parts, halves)
    for d in range(1, parts):
        pieces[d] = lax.ppermute(pieces[d], "mem_y", [(i, (i + d) % parts) for i in range(parts)])
    synthesis = spectral(scalars, spectrum, arrived, legendre)
    returned = swap(synthesis.reshape(sources * parts, quarter, waves, lanes), SPACE + ("mem_y",))
    returned = returned.reshape(sources, parts, quarter, waves, lanes)
    kept, sent = backward(scalars, lift, returned, fourier, pieces, halves)
    came = lax.ppermute(sent, "mem_z", [(0, 1), (1, 0)])
    share = kept.astype(F32) + came.astype(F32)
    rounded = (share / (members * parts * halves - 1)).astype(BF16)
    everyone = jnp.broadcast_to(rounded[None], (parts * halves, *rounded.shape))
    gathered = swap(everyone, ("mem_y", "mem_z"))
    return place(order, gathered.reshape(levels * rows, lons)).reshape(levels, rows, lons)


def solution(mesh):
    torus = Mesh(
        mesh.devices.reshape(4, 4, 2, 4, 2), ("space_0", "space_1", "space_2", "mem_y", "mem_z")
    )
    in_specs = (
        P(("mem_y", "mem_z"), None, SPACE, None),
        P(None, SPACE, None),
        P(),
        P(SPACE, None, None),
        P(SPACE, None),
        P(),
    )
    out_specs = P(None, SPACE, None)
    return jax.shard_map(on_device, mesh=torus, in_specs=in_specs, out_specs=out_specs, check_vma=False)
```

```python
import functools
import math

import jax
import jax.numpy as jnp
import numpy as np
from jax import lax
from jax.experimental import pallas as pl
from jax.experimental.pallas import tpu as pltpu
from jax.sharding import Mesh
from jax.sharding import PartitionSpec as P


NLON = 1536
M = 512
SPACE = ("space_0", "space_1", "space_2")
F32 = jnp.float32
BF16 = jnp.bfloat16
NT = (((1,), (1,)), ((), ()))
TN = (((0,), (0,)), ((), ()))


def angle_tables(block):
    points = np.arange(NLON)[None, :]
    amplitude = math.sqrt(2.0 / NLON)

    def angles(waves):
        return (points * waves[:, None] % NLON) * (2.0 * math.pi / NLON)

    low = angles(np.arange(block))
    high = angles(np.arange(M // block) * block)
    tables = (np.cos(low) * amplitude, np.sin(low) * amplitude, np.cos(high), np.sin(high))
    return [jnp.asarray(t, F32) for t in tables]


def iota2(shape, dim):
    return lax.broadcasted_iota(jnp.int32, shape, dim)


def over(value, size):
    assert size & (size - 1) == 0
    return value >> (size.bit_length() - 1)


def rest_of(value, size):
    assert size & (size - 1) == 0
    return value & (size - 1)


def one_hot(match):
    return jnp.where(match, 1.0, 0.0).astype(BF16)


def build_table(ft_ref, low_c, low_s, high_c, high_s):
    block = low_c.shape[0]

    def build(t, carry):
        hc = high_c[pl.ds(t, 1), :]
        hs = high_s[pl.ds(t, 1), :]
        at = pl.multiple_of(t * block, block)
        ft_ref[pl.ds(at, block), :] = (low_c[...] * hc - low_s[...] * hs).astype(BF16)
        ft_ref[pl.ds(M + at, block), :] = -(low_s[...] * hc + low_c[...] * hs).astype(BF16)
        return carry

    lax.fori_loop(0, M // block, build, 0)


def forward_kernel(modes_ref, low_c, low_s, high_c, high_s, e_hbm, v_hbm, z_hbm, ft, kp, p, y, e, v, z, arrive, leave):
    modes_n, levels = modes_ref.shape
    members = e.shape[0]
    rows = kp.shape[0] // modes_n
    fields = p.shape[0] // rows
    loads = [pltpu.make_async_copy(v_hbm, v, arrive.at[members])]
    for k in range(members):
        loads.append(pltpu.make_async_copy(e_hbm.at[k], e.at[k], arrive.at[k]))
    for load in loads:
        load.start()

    build_table(ft, low_c, low_s, high_c, high_s)
    ra = one_hot(rest_of(iota2((rows * modes_n, modes_n), 0), modes_n) == iota2((rows * modes_n, modes_n), 1))
    la = one_hot(over(iota2((levels, levels * rows), 1), rows) == iota2((levels, levels * rows), 0))
    spread_rows = jnp.dot(ra, modes_ref[...].astype(BF16), preferred_element_type=F32)
    full = jnp.dot(spread_rows.astype(BF16), la, preferred_element_type=F32)
    mask = over(iota2(kp.shape, 0), modes_n) == rest_of(iota2(kp.shape, 1), rows)
    kp[...] = jnp.where(mask, full, 0.0).astype(BF16)

    loads[0].wait()
    for k in range(members):
        loads[1 + k].wait()
        projected = jnp.dot(kp[...], e[k] * v[...], preferred_element_type=F32).astype(BF16)
        for a in range(rows):
            at = a * fields + k * modes_n
            p[at : at + modes_n, :] = projected[a * modes_n : (a + 1) * modes_n]

    lane = iota2((M, 2 * fields), 1)
    wide = 4 * fields
    for chunk in range(rows // 4):
        got = lax.dot_general(
            ft[...], p[chunk * wide : (chunk + 1) * wide, :], NT, preferred_element_type=F32
        )
        for pair in range(2):
            lanes = slice(pair * 2 * fields, (pair + 1) * 2 * fields)
            tc = got[:M, lanes]
            ts = got[M:, lanes]
            a = chunk * 4 + pair * 2
            y[pl.ds(a, M, stride=rows), :] = jnp.where(lane < fields, tc, pltpu.roll(ts, fields, 1))
            y[pl.ds(a + 1, M, stride=rows), :] = jnp.where(lane < fields, pltpu.roll(tc, fields, 1), ts)

    stores = []
    count = leave.shape[0]
    size = z.shape[0] // count
    for i in range(count):
        part = pl.ds(i * size, size)
        z[part, :] = y[part, :].astype(BF16)
        stores.append(pltpu.make_async_copy(z.at[part], z_hbm.at[part], leave.at[i]))
        stores[i].start()
    for store in stores:
        store.wait()


def forward(modes, ensemble, vector):
    members, levels, rows, lons = ensemble.shape
    modes_n = modes.shape[0]
    fields = members * modes_n
    tables = angle_tables(16)
    whole = pl.BlockSpec(memory_space=pltpu.MemorySpace.VMEM)
    outside = pl.BlockSpec(memory_space=pltpu.MemorySpace.HBM)
    return pl.pallas_call(
        forward_kernel,
        in_specs=[whole] * 5 + [outside] * 2,
        out_specs=outside,
        out_shape=jax.ShapeDtypeStruct((M * rows, 2 * fields), BF16),
        scratch_shapes=[
            pltpu.VMEM((2 * M, lons), BF16),
            pltpu.VMEM((rows * modes_n, levels * rows), BF16),
            pltpu.VMEM((rows * fields, lons), BF16),
            pltpu.VMEM((M * rows, 2 * fields), F32),
            pltpu.VMEM((members, levels * rows, lons), BF16),
            pltpu.VMEM((levels * rows, lons), BF16),
            pltpu.VMEM((M * rows, 2 * fields), BF16),
            pltpu.SemaphoreType.DMA((members + 1,)),
            pltpu.SemaphoreType.DMA((8,)),
        ],
        compiler_params=pltpu.CompilerParams(vmem_limit_bytes=62 * 2**20),
        name="forward",
    )(
        modes,
        *tables,
        ensemble.reshape(members, levels * rows, lons),
        vector.reshape(levels * rows, lons),
    )


def divide_kernel(scalars, e_ref, *rest, rows):
    *out_refs, perm = rest
    parts = len(out_refs)
    share = out_refs[0].shape[1]
    per = rows // parts

    @pl.when(pl.program_id(0) == 0)
    def _():
        row = iota2(perm.shape, 0)
        part = rest_of(scalars[2] + over(row, share), parts)
        level = over(rest_of(row, share), per)
        perm[...] = one_hot(iota2(perm.shape, 1) == level * rows + part * per + rest_of(row, per))

    moved = jnp.dot(perm[...], e_ref[0], preferred_element_type=F32).astype(BF16)
    for d, out_ref in enumerate(out_refs):
        out_ref[0] = moved[d * share : (d + 1) * share]


def divide(scalars, ensemble, parts):
    members, levels, rows, lons = ensemble.shape
    height = levels * rows
    share = height // parts
    return pl.pallas_call(
        functools.partial(divide_kernel, rows=rows),
        grid_spec=pltpu.PrefetchScalarGridSpec(
            num_scalar_prefetch=1,
            grid=(members,),
            in_specs=[pl.BlockSpec((1, height, lons), lambda k, _: (k, 0, 0))],
            out_specs=[pl.BlockSpec((1, share, lons), lambda k, _: (k, 0, 0))] * parts,
            scratch_shapes=[pltpu.VMEM((height, height), BF16)],
        ),
        out_shape=[jax.ShapeDtypeStruct((members, share, lons), BF16)] * parts,
        compiler_params=pltpu.CompilerParams(vmem_limit_bytes=62 * 2**20),
        cost_estimate=pl.CostEstimate(flops=10**10, bytes_accessed=2 * 10**7, transcendentals=0),
        name="divide",
    )(scalars, ensemble.reshape(members, height, lons))


def matrices_kernel(modes_ref, low_c, low_s, high_c, high_s, ft_ref, kl, order, *, rows, parts, halves):
    modes_n, levels = modes_ref.shape
    per = rows // parts
    columns = per * modes_n
    share = levels * per
    build_table(ft_ref, low_c, low_s, high_c, high_s)
    row = iota2(order.shape, 0)
    level = over(row, rows)
    lat = rest_of(row, rows)
    half = levels // halves
    source = over(lat, per) * halves + over(level, half)
    wanted = source * (half * per) + rest_of(level, half) * per + rest_of(lat, per)
    order[...] = one_hot(iota2(order.shape, 1) == wanted)
    height, width = kl.shape
    la = one_hot(over(rest_of(iota2((height, levels), 0), share), per) == iota2((height, levels), 1))
    ra = one_hot(rest_of(iota2((modes_n, width), 1), modes_n) == iota2((modes_n, width), 0))
    spread_rows = lax.dot_general(la, modes_ref[...].astype(BF16), NT, preferred_element_type=F32)
    full = jnp.dot(spread_rows.astype(BF16), ra, preferred_element_type=F32)
    row = iota2(kl.shape, 0)
    col = iota2(kl.shape, 1)
    mask = (over(row, share) == over(col, columns)) & (
        rest_of(row, per) == over(rest_of(col, columns), modes_n)
    )
    kl[...] = jnp.where(mask, full, 0.0).astype(BF16)


def matrices(modes, members, rows, parts, halves):
    modes_n, levels = modes.shape
    per = rows // parts
    tables = angle_tables(16)
    whole = pl.BlockSpec(memory_space=pltpu.MemorySpace.VMEM)
    return pl.pallas_call(
        functools.partial(matrices_kernel, rows=rows, parts=parts, halves=halves),
        in_specs=[whole] * 5,
        out_specs=[whole] * 3,
        out_shape=[
            jax.ShapeDtypeStruct((2 * M, NLON), BF16),
            jax.ShapeDtypeStruct((members * levels * per, members * per * modes_n), BF16),
            jax.ShapeDtypeStruct((levels * rows, levels * rows), BF16),
        ],
        compiler_params=pltpu.CompilerParams(vmem_limit_bytes=62 * 2**20),
        cost_estimate=pl.CostEstimate(flops=10**9, bytes_accessed=4 * 10**6, transcendentals=0),
        name="matrices",
    )(modes, *tables)


def spectral_kernel(scalars, spectrum_ref, x_hbm, l_hbm, out_hbm, s, x, l, z, arrive_x, arrive_l, leave):
    sources, waves, rows, lanes = x.shape
    degrees = l.shape[2]
    height = sources * rows
    groups = arrive_x.shape[0]
    per = waves // groups
    loads = []
    for i in range(groups):
        part = pl.ds(i * per, per)
        loads.append(
            (
                pltpu.make_async_copy(x_hbm.at[:, part], x.at[:, part], arrive_x.at[i]),
                pltpu.make_async_copy(l_hbm.at[part], l.at[part], arrive_l.at[i]),
            )
        )
        for load in loads[i]:
            load.start()
    for i in range(groups):
        for load in loads[i]:
            load.wait()
        for m in range(i * per, (i + 1) * per):
            own = x[:, m].reshape(height, lanes)
            harmonic = lax.dot_general(own, l[m], TN, preferred_element_type=F32)
            total = scalars[1] + m + iota2((1, degrees), 1)
            factor = jnp.where(total <= scalars[0], spectrum_ref[m : m + 1, :], 0.0)
            weighted = (harmonic * factor).astype(BF16)
            back = lax.dot_general(l[m], weighted, NT, preferred_element_type=F32)
            s[pl.ds(m, height, stride=waves), :] = back
    stores = []
    count = leave.shape[0]
    size = height * waves // count
    for i in range(count):
        part = pl.ds(i * size, size)
        z[part, :] = s[part, :].astype(BF16)
        stores.append(pltpu.make_async_copy(z.at[part], out_hbm.at[part], leave.at[i]))
        stores[i].start()
    for store in stores:
        store.wait()


def spectral(scalars, spectrum, arrived, legendre):
    sources, waves, rows, lanes = arrived.shape
    height = sources * rows * waves
    outside = pl.BlockSpec(memory_space=pltpu.MemorySpace.HBM)
    return pl.pallas_call(
        spectral_kernel,
        in_specs=[
            pl.BlockSpec(memory_space=pltpu.MemorySpace.SMEM),
            pl.BlockSpec(memory_space=pltpu.MemorySpace.VMEM),
            outside,
            outside,
        ],
        out_specs=outside,
        out_shape=jax.ShapeDtypeStruct((height, lanes), BF16),
        scratch_shapes=[
            pltpu.VMEM((height, lanes), F32),
            pltpu.VMEM(arrived.shape, BF16),
            pltpu.VMEM(legendre.shape, BF16),
            pltpu.VMEM((height, lanes), BF16),
            pltpu.SemaphoreType.DMA((4,)),
            pltpu.SemaphoreType.DMA((4,)),
            pltpu.SemaphoreType.DMA((8,)),
        ],
        compiler_params=pltpu.CompilerParams(vmem_limit_bytes=50 * 2**20),
        name="spectral",
    )(scalars, spectrum, arrived, legendre)


def backward_kernel(scalars, kl_ref, r_ref, ft_ref, *rest):
    *e_refs, kept_ref, sent_ref, g, sums = rest
    sources, parts, rows, waves, lanes = r_ref.shape
    members, share = e_refs[0].shape[:2]
    fields = lanes // 2
    modes_n = fields // members
    columns = rows * modes_n

    @pl.when(pl.program_id(0) == 0)
    def _():
        for d in range(parts):
            source = rest_of(scalars[2] + parts - d, parts)
            for a in range(rows):
                flipped = r_ref[:, source, a].reshape(sources * waves, lanes).T
                for r in range(2):
                    for k in range(members):
                        at = r * fields + k * modes_n
                        to = (d * members + k) * columns + a * modes_n
                        g[to : to + modes_n, r * M : (r + 1) * M] = flipped[at : at + modes_n]

    spread = jnp.dot(g[...], ft_ref[...], preferred_element_type=F32).astype(BF16)
    group = members * columns
    total = None
    for d in range(parts):
        lifted = jnp.dot(kl_ref[...], spread[d * group : (d + 1) * group], preferred_element_type=F32)
        for k in range(members):
            term = e_refs[d][k].astype(F32) * lifted[k * share : (k + 1) * share]
            total = term if total is None else total + term
    sums[...] = total.astype(BF16)
    half = kept_ref.shape[0]
    at = scalars[3] * half
    kept_ref[...] = sums[pl.ds(pl.multiple_of(at, half), half), :]
    sent_ref[...] = sums[pl.ds(pl.multiple_of(half - at, half), half), :]


def backward(scalars, lift, returned, fourier, pieces, halves):
    _, parts, _, _, _ = returned.shape
    members, share, lons = pieces[0].shape
    chunk = 512
    half = share // halves
    return pl.pallas_call(
        backward_kernel,
        grid_spec=pltpu.PrefetchScalarGridSpec(
            num_scalar_prefetch=1,
            grid=(lons // chunk,),
            in_specs=[
                pl.BlockSpec(lift.shape, lambda i, _: (0, 0)),
                pl.BlockSpec(returned.shape, lambda i, _: (0, 0, 0, 0, 0)),
                pl.BlockSpec((2 * M, chunk), lambda i, _: (0, i)),
            ]
            + [pl.BlockSpec((members, share, chunk), lambda i, _: (0, 0, i))] * parts,
            out_specs=[pl.BlockSpec((half, chunk), lambda i, _: (0, i))] * halves,
            scratch_shapes=[
                pltpu.VMEM((parts * lift.shape[1], 2 * M), BF16),
                pltpu.VMEM((share, chunk), BF16),
            ],
        ),
        out_shape=[jax.ShapeDtypeStruct((half, lons), BF16)] * halves,
        compiler_params=pltpu.CompilerParams(vmem_limit_bytes=50 * 2**20),
        name="backward",
    )(scalars, lift, returned, fourier, *pieces)


def place_kernel(order_ref, x_ref, out_ref):
    out_ref[...] = jnp.dot(order_ref[...], x_ref[...], preferred_element_type=F32).astype(BF16)


def place(order, gathered):
    height, lons = gathered.shape
    chunk = 512
    return pl.pallas_call(
        place_kernel,
        grid=(lons // chunk,),
        in_specs=[
            pl.BlockSpec(order.shape, lambda i: (0, 0)),
            pl.BlockSpec((height, chunk), lambda i: (0, i)),
        ],
        out_specs=pl.BlockSpec((height, chunk), lambda i: (0, i)),
        out_shape=jax.ShapeDtypeStruct((height, lons), BF16),
        compiler_params=pltpu.CompilerParams(vmem_limit_bytes=16 * 2**20),
        name="place",
    )(order, gathered)


def swap(blocks, axes):
    return lax.all_to_all(blocks, axes, 0, 0, tiled=True)


def on_device(ensemble, vector, modes, legendre, spectrum, truncation):
    members, levels, rows, lons = ensemble.shape
    waves = legendre.shape[0]
    sources = lax.axis_size(SPACE)
    parts = lax.axis_size("mem_y")
    halves = lax.axis_size("mem_z")
    lanes = 2 * members * modes.shape[0]
    quarter = rows // parts
    first_wave = lax.axis_index(SPACE) * waves
    places = [first_wave, lax.axis_index("mem_y"), lax.axis_index("mem_z")]
    scalars = jnp.stack([truncation[0], *[i.astype(jnp.int32) for i in places]])
    zonal = forward(modes, ensemble, vector)
    arrived = swap(zonal.reshape(sources, waves, rows, lanes), SPACE)
    held, _ = lax.optimization_barrier((ensemble, zonal))
    pieces = list(divide(scalars, held, parts))
    for d in range(1, parts):
        pieces[d] = lax.ppermute(pieces[d], "mem_y", [(i, (i + d) % parts) for i in range(parts)])
    fourier, lift, order = matrices(modes, members, rows, parts, halves)
    synthesis = spectral(scalars, spectrum, arrived, legendre)
    returned = swap(synthesis.reshape(sources * parts, quarter, waves, lanes), SPACE + ("mem_y",))
    returned = returned.reshape(sources, parts, quarter, waves, lanes)
    kept, sent = backward(scalars, lift, returned, fourier, pieces, halves)
    came = lax.ppermute(sent, "mem_z", [(0, 1), (1, 0)])
    share = kept.astype(F32) + came.astype(F32)
    rounded = (share / (members * parts * halves - 1)).astype(BF16)
    everyone = jnp.broadcast_to(rounded[None], (parts * halves, *rounded.shape))
    gathered = swap(everyone, ("mem_y", "mem_z"))
    return place(order, gathered.reshape(levels * rows, lons)).reshape(levels, rows, lons)


def solution(mesh):
    torus = Mesh(
        mesh.devices.reshape(4, 4, 2, 4, 2), ("space_0", "space_1", "space_2", "mem_y", "mem_z")
    )
    in_specs = (
        P(("mem_y", "mem_z"), None, SPACE, None),
        P(None, SPACE, None),
        P(),
        P(SPACE, None, None),
        P(SPACE, None),
        P(),
    )
    out_specs = P(None, SPACE, None)
    return jax.shard_map(on_device, mesh=torus, in_specs=in_specs, out_specs=out_specs, check_vma=False)
```

```python
import functools
import math

import jax
import jax.numpy as jnp
import numpy as np
from jax import lax
from jax.experimental import pallas as pl
from jax.experimental.pallas import tpu as pltpu
from jax.sharding import Mesh
from jax.sharding import PartitionSpec as P


NLON = 1536
M = 512
SPACE = ("space_0", "space_1", "space_2")
F32 = jnp.float32
BF16 = jnp.bfloat16
NT = (((1,), (1,)), ((), ()))
TN = (((0,), (0,)), ((), ()))


def angle_tables(block):
    points = np.arange(NLON)[None, :]
    amplitude = math.sqrt(2.0 / NLON)

    def angles(waves):
        return (points * waves[:, None] % NLON) * (2.0 * math.pi / NLON)

    low = angles(np.arange(block))
    high = angles(np.arange(M // block) * block)
    tables = (np.cos(low) * amplitude, np.sin(low) * amplitude, np.cos(high), np.sin(high))
    return [jnp.asarray(t, F32) for t in tables]


def iota2(shape, dim):
    return lax.broadcasted_iota(jnp.int32, shape, dim)


def over(value, size):
    assert size & (size - 1) == 0
    return value >> (size.bit_length() - 1)


def rest_of(value, size):
    assert size & (size - 1) == 0
    return value & (size - 1)


def one_hot(match):
    return jnp.where(match, 1.0, 0.0).astype(BF16)


def build_table(ft_ref, low_c, low_s, high_c, high_s):
    block = low_c.shape[0]

    def build(t, carry):
        hc = high_c[pl.ds(t, 1), :]
        hs = high_s[pl.ds(t, 1), :]
        at = pl.multiple_of(t * block, block)
        ft_ref[pl.ds(at, block), :] = (low_c[...] * hc - low_s[...] * hs).astype(BF16)
        ft_ref[pl.ds(M + at, block), :] = -(low_s[...] * hc + low_c[...] * hs).astype(BF16)
        return carry

    lax.fori_loop(0, M // block, build, 0)


def forward_kernel(modes_ref, low_c, low_s, high_c, high_s, e_hbm, v_hbm, z_hbm, ft, kp, p, y, e, v, z, arrive, leave):
    modes_n, levels = modes_ref.shape
    members = e.shape[0]
    rows = kp.shape[0] // modes_n
    fields = p.shape[0] // rows
    loads = [pltpu.make_async_copy(v_hbm, v, arrive.at[members])]
    for k in range(members):
        loads.append(pltpu.make_async_copy(e_hbm.at[k], e.at[k], arrive.at[k]))
    for load in loads:
        load.start()

    build_table(ft, low_c, low_s, high_c, high_s)
    ra = one_hot(rest_of(iota2((rows * modes_n, modes_n), 0), modes_n) == iota2((rows * modes_n, modes_n), 1))
    la = one_hot(over(iota2((levels, levels * rows), 1), rows) == iota2((levels, levels * rows), 0))
    spread_rows = jnp.dot(ra, modes_ref[...].astype(BF16), preferred_element_type=F32)
    full = jnp.dot(spread_rows.astype(BF16), la, preferred_element_type=F32)
    mask = over(iota2(kp.shape, 0), modes_n) == rest_of(iota2(kp.shape, 1), rows)
    kp[...] = jnp.where(mask, full, 0.0).astype(BF16)

    loads[0].wait()
    for k in range(members):
        loads[1 + k].wait()
        projected = jnp.dot(kp[...], e[k] * v[...], preferred_element_type=F32).astype(BF16)
        for a in range(rows):
            at = a * fields + k * modes_n
            p[at : at + modes_n, :] = projected[a * modes_n : (a + 1) * modes_n]

    lane = iota2((M, 2 * fields), 1)
    wide = 4 * fields
    for chunk in range(rows // 4):
        got = lax.dot_general(
            ft[...], p[chunk * wide : (chunk + 1) * wide, :], NT, preferred_element_type=F32
        )
        for pair in range(2):
            lanes = slice(pair * 2 * fields, (pair + 1) * 2 * fields)
            tc = got[:M, lanes]
            ts = got[M:, lanes]
            a = chunk * 4 + pair * 2
            y[pl.ds(a, M, stride=rows), :] = jnp.where(lane < fields, tc, pltpu.roll(ts, fields, 1))
            y[pl.ds(a + 1, M, stride=rows), :] = jnp.where(lane < fields, pltpu.roll(tc, fields, 1), ts)

    stores = []
    count = leave.shape[0]
    size = z.shape[0] // count
    for i in range(count):
        part = pl.ds(i * size, size)
        z[part, :] = y[part, :].astype(BF16)
        stores.append(pltpu.make_async_copy(z.at[part], z_hbm.at[part], leave.at[i]))
        stores[i].start()
    for store in stores:
        store.wait()


def forward(modes, ensemble, vector):
    members, levels, rows, lons = ensemble.shape
    modes_n = modes.shape[0]
    fields = members * modes_n
    tables = angle_tables(16)
    whole = pl.BlockSpec(memory_space=pltpu.MemorySpace.VMEM)
    outside = pl.BlockSpec(memory_space=pltpu.MemorySpace.HBM)
    return pl.pallas_call(
        forward_kernel,
        in_specs=[whole] * 5 + [outside] * 2,
        out_specs=outside,
        out_shape=jax.ShapeDtypeStruct((M * rows, 2 * fields), BF16),
        scratch_shapes=[
            pltpu.VMEM((2 * M, lons), BF16),
            pltpu.VMEM((rows * modes_n, levels * rows), BF16),
            pltpu.VMEM((rows * fields, lons), BF16),
            pltpu.VMEM((M * rows, 2 * fields), F32),
            pltpu.VMEM((members, levels * rows, lons), BF16),
            pltpu.VMEM((levels * rows, lons), BF16),
            pltpu.VMEM((M * rows, 2 * fields), BF16),
            pltpu.SemaphoreType.DMA((members + 1,)),
            pltpu.SemaphoreType.DMA((8,)),
        ],
        compiler_params=pltpu.CompilerParams(vmem_limit_bytes=62 * 2**20),
        name="forward",
    )(
        modes,
        *tables,
        ensemble.reshape(members, levels * rows, lons),
        vector.reshape(levels * rows, lons),
    )


def divide_kernel(scalars, e_ref, out_ref, perm, *, rows, parts, up):
    per = rows // parts

    @pl.when(pl.program_id(0) == 0)
    def _():
        row = iota2(perm.shape, 0)
        part = rest_of(scalars[2] + up, parts)
        perm[...] = one_hot(iota2(perm.shape, 1) == over(row, per) * rows + part * per + rest_of(row, per))

    out_ref[0] = jnp.dot(perm[...], e_ref[0], preferred_element_type=F32).astype(BF16)


def divide(scalars, ensemble, parts, up):
    members, levels, rows, lons = ensemble.shape
    height = levels * rows
    share = height // parts
    return pl.pallas_call(
        functools.partial(divide_kernel, rows=rows, parts=parts, up=up),
        grid_spec=pltpu.PrefetchScalarGridSpec(
            num_scalar_prefetch=1,
            grid=(members,),
            in_specs=[pl.BlockSpec((1, height, lons), lambda k, _: (k, 0, 0))],
            out_specs=pl.BlockSpec((1, share, lons), lambda k, _: (k, 0, 0)),
            scratch_shapes=[pltpu.VMEM((share, height), BF16)],
        ),
        out_shape=jax.ShapeDtypeStruct((members, share, lons), BF16),
        compiler_params=pltpu.CompilerParams(vmem_limit_bytes=62 * 2**20),
        cost_estimate=pl.CostEstimate(flops=25 * 10**8, bytes_accessed=8 * 10**6, transcendentals=0),
        name="divide",
    )(scalars, ensemble.reshape(members, height, lons))


def matrices_kernel(modes_ref, low_c, low_s, high_c, high_s, ft_ref, kl, order, *, rows, parts, halves):
    modes_n, levels = modes_ref.shape
    per = rows // parts
    columns = per * modes_n
    share = levels * per
    build_table(ft_ref, low_c, low_s, high_c, high_s)
    row = iota2(order.shape, 0)
    level = over(row, rows)
    lat = rest_of(row, rows)
    half = levels // halves
    source = over(lat, per) * halves + over(level, half)
    wanted = source * (half * per) + rest_of(level, half) * per + rest_of(lat, per)
    order[...] = one_hot(iota2(order.shape, 1) == wanted)
    height, width = kl.shape
    la = one_hot(over(rest_of(iota2((height, levels), 0), share), per) == iota2((height, levels), 1))
    ra = one_hot(rest_of(iota2((modes_n, width), 1), modes_n) == iota2((modes_n, width), 0))
    spread_rows = lax.dot_general(la, modes_ref[...].astype(BF16), NT, preferred_element_type=F32)
    full = jnp.dot(spread_rows.astype(BF16), ra, preferred_element_type=F32)
    row = iota2(kl.shape, 0)
    col = iota2(kl.shape, 1)
    mask = (over(row, share) == over(col, columns)) & (
        rest_of(row, per) == over(rest_of(col, columns), modes_n)
    )
    kl[...] = jnp.where(mask, full, 0.0).astype(BF16)


def matrices(modes, members, rows, parts, halves):
    modes_n, levels = modes.shape
    per = rows // parts
    tables = angle_tables(16)
    whole = pl.BlockSpec(memory_space=pltpu.MemorySpace.VMEM)
    return pl.pallas_call(
        functools.partial(matrices_kernel, rows=rows, parts=parts, halves=halves),
        in_specs=[whole] * 5,
        out_specs=[whole] * 3,
        out_shape=[
            jax.ShapeDtypeStruct((2 * M, NLON), BF16),
            jax.ShapeDtypeStruct((members * levels * per, members * per * modes_n), BF16),
            jax.ShapeDtypeStruct((levels * rows, levels * rows), BF16),
        ],
        compiler_params=pltpu.CompilerParams(vmem_limit_bytes=62 * 2**20),
        cost_estimate=pl.CostEstimate(flops=10**9, bytes_accessed=4 * 10**6, transcendentals=0),
        name="matrices",
    )(modes, *tables)


def spectral_kernel(scalars, spectrum_ref, x_hbm, l_hbm, out_hbm, s, x, l, z, arrive_x, arrive_l, leave):
    sources, waves, rows, lanes = x.shape
    degrees = l.shape[2]
    height = sources * rows
    groups = arrive_x.shape[0]
    per = waves // groups
    loads = []
    for i in range(groups):
        part = pl.ds(i * per, per)
        loads.append(
            (
                pltpu.make_async_copy(x_hbm.at[:, part], x.at[:, part], arrive_x.at[i]),
                pltpu.make_async_copy(l_hbm.at[part], l.at[part], arrive_l.at[i]),
            )
        )
        for load in loads[i]:
            load.start()
    for i in range(groups):
        for load in loads[i]:
            load.wait()
        for m in range(i * per, (i + 1) * per):
            own = x[:, m].reshape(height, lanes)
            harmonic = lax.dot_general(own, l[m], TN, preferred_element_type=F32)
            total = scalars[1] + m + iota2((1, degrees), 1)
            factor = jnp.where(total <= scalars[0], spectrum_ref[m : m + 1, :], 0.0)
            weighted = (harmonic * factor).astype(BF16)
            back = lax.dot_general(l[m], weighted, NT, preferred_element_type=F32)
            s[pl.ds(m, height, stride=waves), :] = back
    stores = []
    count = leave.shape[0]
    size = height * waves // count
    for i in range(count):
        part = pl.ds(i * size, size)
        z[part, :] = s[part, :].astype(BF16)
        stores.append(pltpu.make_async_copy(z.at[part], out_hbm.at[part], leave.at[i]))
        stores[i].start()
    for store in stores:
        store.wait()


def spectral(scalars, spectrum, arrived, legendre):
    sources, waves, rows, lanes = arrived.shape
    height = sources * rows * waves
    outside = pl.BlockSpec(memory_space=pltpu.MemorySpace.HBM)
    return pl.pallas_call(
        spectral_kernel,
        in_specs=[
            pl.BlockSpec(memory_space=pltpu.MemorySpace.SMEM),
            pl.BlockSpec(memory_space=pltpu.MemorySpace.VMEM),
            outside,
            outside,
        ],
        out_specs=outside,
        out_shape=jax.ShapeDtypeStruct((height, lanes), BF16),
        scratch_shapes=[
            pltpu.VMEM((height, lanes), F32),
            pltpu.VMEM(arrived.shape, BF16),
            pltpu.VMEM(legendre.shape, BF16),
            pltpu.VMEM((height, lanes), BF16),
            pltpu.SemaphoreType.DMA((4,)),
            pltpu.SemaphoreType.DMA((4,)),
            pltpu.SemaphoreType.DMA((8,)),
        ],
        compiler_params=pltpu.CompilerParams(vmem_limit_bytes=50 * 2**20),
        name="spectral",
    )(scalars, spectrum, arrived, legendre)


def backward_kernel(scalars, kl_ref, r_ref, ft_ref, *rest):
    *e_refs, kept_ref, sent_ref, g, sums = rest
    sources, parts, rows, waves, lanes = r_ref.shape
    members, share = e_refs[0].shape[:2]
    fields = lanes // 2
    modes_n = fields // members
    columns = rows * modes_n

    @pl.when(pl.program_id(0) == 0)
    def _():
        for d in range(parts):
            source = rest_of(scalars[2] + parts - d, parts)
            for a in range(rows):
                flipped = r_ref[:, source, a].reshape(sources * waves, lanes).T
                for r in range(2):
                    for k in range(members):
                        at = r * fields + k * modes_n
                        to = (d * members + k) * columns + a * modes_n
                        g[to : to + modes_n, r * M : (r + 1) * M] = flipped[at : at + modes_n]

    spread = jnp.dot(g[...], ft_ref[...], preferred_element_type=F32).astype(BF16)
    group = members * columns
    total = None
    for d in range(parts):
        lifted = jnp.dot(kl_ref[...], spread[d * group : (d + 1) * group], preferred_element_type=F32)
        for k in range(members):
            term = e_refs[d][k].astype(F32) * lifted[k * share : (k + 1) * share]
            total = term if total is None else total + term
    sums[...] = total.astype(BF16)
    half = kept_ref.shape[0]
    at = scalars[3] * half
    kept_ref[...] = sums[pl.ds(pl.multiple_of(at, half), half), :]
    sent_ref[...] = sums[pl.ds(pl.multiple_of(half - at, half), half), :]


def backward(scalars, lift, returned, fourier, pieces, halves):
    _, parts, _, _, _ = returned.shape
    members, share, lons = pieces[0].shape
    chunk = 512
    half = share // halves
    return pl.pallas_call(
        backward_kernel,
        grid_spec=pltpu.PrefetchScalarGridSpec(
            num_scalar_prefetch=1,
            grid=(lons // chunk,),
            in_specs=[
                pl.BlockSpec(lift.shape, lambda i, _: (0, 0)),
                pl.BlockSpec(returned.shape, lambda i, _: (0, 0, 0, 0, 0)),
                pl.BlockSpec((2 * M, chunk), lambda i, _: (0, i)),
            ]
            + [pl.BlockSpec((members, share, chunk), lambda i, _: (0, 0, i))] * parts,
            out_specs=[pl.BlockSpec((half, chunk), lambda i, _: (0, i))] * halves,
            scratch_shapes=[
                pltpu.VMEM((parts * lift.shape[1], 2 * M), BF16),
                pltpu.VMEM((share, chunk), BF16),
            ],
        ),
        out_shape=[jax.ShapeDtypeStruct((half, lons), BF16)] * halves,
        compiler_params=pltpu.CompilerParams(vmem_limit_bytes=50 * 2**20),
        name="backward",
    )(scalars, lift, returned, fourier, *pieces)


def place_kernel(order_ref, x_ref, out_ref):
    out_ref[...] = jnp.dot(order_ref[...], x_ref[...], preferred_element_type=F32).astype(BF16)


def place(order, gathered):
    height, lons = gathered.shape
    chunk = 512
    return pl.pallas_call(
        place_kernel,
        grid=(lons // chunk,),
        in_specs=[
            pl.BlockSpec(order.shape, lambda i: (0, 0)),
            pl.BlockSpec((height, chunk), lambda i: (0, i)),
        ],
        out_specs=pl.BlockSpec((height, chunk), lambda i: (0, i)),
        out_shape=jax.ShapeDtypeStruct((height, lons), BF16),
        compiler_params=pltpu.CompilerParams(vmem_limit_bytes=16 * 2**20),
        name="place",
    )(order, gathered)


def swap(blocks, axes):
    return lax.all_to_all(blocks, axes, 0, 0, tiled=True)


def on_device(ensemble, vector, modes, legendre, spectrum, truncation):
    members, levels, rows, lons = ensemble.shape
    waves = legendre.shape[0]
    sources = lax.axis_size(SPACE)
    parts = lax.axis_size("mem_y")
    halves = lax.axis_size("mem_z")
    lanes = 2 * members * modes.shape[0]
    quarter = rows // parts
    first_wave = lax.axis_index(SPACE) * waves
    places = [first_wave, lax.axis_index("mem_y"), lax.axis_index("mem_z")]
    scalars = jnp.stack([truncation[0], *[i.astype(jnp.int32) for i in places]])
    zonal = forward(modes, ensemble, vector)
    arrived = swap(zonal.reshape(sources, waves, rows, lanes), SPACE)
    held, _ = lax.optimization_barrier((ensemble, zonal))
    pieces = [None] * parts
    for d in (2, 1, 3, 0):
        pieces[d] = divide(scalars, held, parts, d)
        if d:
            pieces[d] = lax.ppermute(pieces[d], "mem_y", [(i, (i + d) % parts) for i in range(parts)])
    fourier, lift, order = matrices(modes, members, rows, parts, halves)
    synthesis = spectral(scalars, spectrum, arrived, legendre)
    returned = swap(synthesis.reshape(sources * parts, quarter, waves, lanes), SPACE + ("mem_y",))
    returned = returned.reshape(sources, parts, quarter, waves, lanes)
    kept, sent = backward(scalars, lift, returned, fourier, pieces, halves)
    came = lax.ppermute(sent, "mem_z", [(0, 1), (1, 0)])
    share = kept.astype(F32) + came.astype(F32)
    rounded = (share / (members * parts * halves - 1)).astype(BF16)
    everyone = jnp.broadcast_to(rounded[None], (parts * halves, *rounded.shape))
    gathered = swap(everyone, ("mem_y", "mem_z"))
    return place(order, gathered.reshape(levels * rows, lons)).reshape(levels, rows, lons)


def solution(mesh):
    torus = Mesh(
        mesh.devices.reshape(4, 4, 2, 4, 2), ("space_0", "space_1", "space_2", "mem_y", "mem_z")
    )
    in_specs = (
        P(("mem_y", "mem_z"), None, SPACE, None),
        P(None, SPACE, None),
        P(),
        P(SPACE, None, None),
        P(SPACE, None),
        P(),
    )
    out_specs = P(None, SPACE, None)
    return jax.shard_map(on_device, mesh=torus, in_specs=in_specs, out_specs=out_specs, check_vma=False)
```
